8 devices in a mesh: depth: 2 (over z, y), col: 2 (over x), row: 2 (over core).
Axes of the slice: x: 2, y: 2, z: 1, core: 2. Of those that a mesh axis runs over, the one named last changes fastest.
Arguments:
- tokens: bfloat16 [8192, 2048], P(('depth', 'row'), 'col')
- w_in: bfloat16 [2048, 16384], P('row', 'col')
- w_out: bfloat16 [16384, 2048], P('row', 'col')
- grad_y: bfloat16 [8192, 2048], P(('depth', 'row'), 'col')
Outputs:
- output 1: bfloat16 [8192, 2048], P(('depth', 'row'), 'col')
- output 2: bfloat16 [8192, 2048], P(('depth', 'row'), 'col')
- output 3: float32 [2048, 16384], P('row', 'col')
- output 4: float32 [16384, 2048], P('row', 'col')
All inputs are finite; a program needn't handle non-finite values.
Results may differ from the reference program's by a relative error of at most 0.00115.
Values are sent between devices in bfloat16 or wider.
A program may use at most 1 GiB of HBM per device.

```python
import jax
import jax.numpy as jnp
from jax import lax

TOKENS = 8192
HIDDEN = 2048
FFN_WIDTH = 16384
BLOCK_ROWS = 2048


def setup_inputs(seed: int = 0) -> dict:
    base_key = jax.random.key(seed)
    key_tok, key_in, key_out, key_grad = jax.random.split(base_key, 4)
    tokens = jax.random.normal(key_tok, (TOKENS, HIDDEN), jnp.float32).astype(jnp.bfloat16)
    w_in = (jax.random.normal(key_in, (HIDDEN, FFN_WIDTH), jnp.float32) * HIDDEN ** -0.5).astype(jnp.bfloat16)
    w_out = (jax.random.normal(key_out, (FFN_WIDTH, HIDDEN), jnp.float32) * FFN_WIDTH ** -0.5).astype(jnp.bfloat16)
    grad_y = jax.random.normal(key_grad, (TOKENS, HIDDEN), jnp.float32).astype(jnp.bfloat16)
    return {"tokens": tokens, "w_in": w_in, "w_out": w_out, "grad_y": grad_y}


def gelu_tanh(pre_act):
    return jax.nn.gelu(pre_act, approximate=True)


def block_terms(tok_blk, grad_blk, w_in, w_out):
    pre_act = jnp.dot(tok_blk, w_in, preferred_element_type=jnp.float32)
    hidden = gelu_tanh(pre_act).astype(jnp.bfloat16)
    y_blk = jnp.dot(hidden, w_out, preferred_element_type=jnp.float32).astype(jnp.bfloat16)
    d_hidden = jnp.dot(grad_blk, w_out.T, preferred_element_type=jnp.float32)
    gelu_back = jax.vjp(gelu_tanh, pre_act)[1]
    d_pre = gelu_back(d_hidden)[0].astype(jnp.bfloat16)
    dx_blk = jnp.dot(d_pre, w_in.T, preferred_element_type=jnp.float32).astype(jnp.bfloat16)
    dw_in = jnp.dot(tok_blk.T, d_pre, preferred_element_type=jnp.float32)
    dw_out = jnp.dot(hidden.T, grad_blk, preferred_element_type=jnp.float32)
    return y_blk, dx_blk, dw_in, dw_out


def reference(tokens, w_in, w_out, grad_y):
    n_blocks = TOKENS // BLOCK_ROWS
    tok_blocks = tokens.reshape(n_blocks, BLOCK_ROWS, HIDDEN)
    grad_blocks = grad_y.reshape(n_blocks, BLOCK_ROWS, HIDDEN)

    def scan_body(acc_pair, blk_pair):
        y_blk, dx_blk, dw_in, dw_out = block_terms(blk_pair[0], blk_pair[1], w_in, w_out)
        return (acc_pair[0] + dw_in, acc_pair[1] + dw_out), (y_blk, dx_blk)

    zero_acc = (jnp.zeros((HIDDEN, FFN_WIDTH), jnp.float32), jnp.zeros((FFN_WIDTH, HIDDEN), jnp.float32))
    grad_sums, outs_pair = lax.scan(scan_body, zero_acc, (tok_blocks, grad_blocks))
    mlp_out = outs_pair[0].reshape(TOKENS, HIDDEN)
    grad_x = outs_pair[1].reshape(TOKENS, HIDDEN)
    return (mlp_out, grad_x, grad_sums[0], grad_sums[1])
```

```python
import jax
import jax.numpy as jnp
from jax import lax
from jax.experimental import pallas as pl
from jax.experimental.pallas import tpu as pltpu
from jax.sharding import PartitionSpec as P


SWAP = [(0, 1), (1, 0)]


def gelu_tanh(pre_act):
    return jax.nn.gelu(pre_act, approximate=True)


def dot(lhs, rhs, lc, rc):
    return lax.dot_general(lhs, rhs, (((lc,), (rc,)), ((), ())), preferred_element_type=jnp.float32)


def part(arr, idx, size, axis):
    return lax.dynamic_slice_in_dim(arr, idx * size, size, axis)


def after(val, *deps):
    return lax.optimization_barrier((val,) + deps)[0]


def join_cols(mine, other, idx):
    rows, cols = mine.shape
    step = 256

    def body(idx_ref, mine_ref, other_ref, out_ref):
        @pl.when(idx_ref[0] == 0)
        def _():
            out_ref[:, :cols] = mine_ref[...]
            out_ref[:, cols:] = other_ref[...]

        @pl.when(idx_ref[0] != 0)
        def _():
            out_ref[:, :cols] = other_ref[...]
            out_ref[:, cols:] = mine_ref[...]

    return pl.pallas_call(
        body,
        out_shape=jax.ShapeDtypeStruct((rows, 2 * cols), mine.dtype),
        grid_spec=pltpu.PrefetchScalarGridSpec(
            num_scalar_prefetch=1,
            grid=(rows // step,),
            in_specs=[pl.BlockSpec((step, cols), lambda i, s: (i, 0))] * 2,
            out_specs=pl.BlockSpec((step, 2 * cols), lambda i, s: (i, 0)),
        ),
        cost_estimate=pl.CostEstimate(flops=rows * cols * 400, bytes_accessed=4 * rows * cols * mine.dtype.itemsize, transcendentals=0),
    )(idx[None], mine, other)


def lay_rows(pieces, places, n_rows, step):
    cols, dtype = pieces[0].shape[1], pieces[0].dtype
    sizes = [p.shape[0] // step for p in pieces]

    def body(place_ref, *refs):
        out_ref = refs[-1]
        at = pl.program_id(0)
        for k, size in enumerate(sizes):
            @pl.when((place_ref[k] >= 0) & (at >= place_ref[k]) & (at < place_ref[k] + size))
            def _(k=k):
                out_ref[...] = refs[k][...]

    def in_map(k, size):
        def index(at, place_ref):
            return (jnp.where(place_ref[k] < 0, 0, jnp.clip(at - place_ref[k], 0, size - 1)), 0)

        return index

    return pl.pallas_call(
        body,
        out_shape=jax.ShapeDtypeStruct((n_rows, cols), dtype),
        grid_spec=pltpu.PrefetchScalarGridSpec(
            num_scalar_prefetch=1,
            grid=(n_rows // step,),
            in_specs=[pl.BlockSpec((step, cols), in_map(k, size)) for k, size in enumerate(sizes)],
            out_specs=pl.BlockSpec((step, cols), lambda at, place_ref: (at, 0)),
        ),
        cost_estimate=pl.CostEstimate(flops=n_rows * cols * 400, bytes_accessed=2 * n_rows * cols * dtype.itemsize, transcendentals=0),
    )(places.astype(jnp.int32), *pieces)


def lay_dw2(own, own_core, oth, oth_core, stay, r, inner):
    step = 256
    whole = own.shape[0] // step
    piece = oth[0].shape[0] // step
    own_places = jnp.stack((whole * r, whole * (1 - r)))
    oth_places = jnp.concatenate((whole * r + piece * inner, whole * (1 - r) + piece * inner))
    places = jnp.concatenate((jnp.where(stay, own_places, -1), jnp.where(stay, -1, oth_places)))
    return lay_rows([own, own_core, *oth, *oth_core], places, 2 * own.shape[0], step)


def solution(mesh):
    act_spec = P(("depth", "row"), "col")
    weight_spec = P("row", "col")

    def step_body(tok, w_in, w_out, grad):
        d, c, r = lax.axis_index("depth"), lax.axis_index("col"), lax.axis_index("row")
        hid = tok.shape[1]
        ffn = w_in.shape[1] // 2
        half = ffn // 2

        def swap(v, axis):
            return lax.ppermute(v, axis, SWAP)

        def cores(v):
            return lax.all_gather(v, "row", axis=0, tiled=True)

        tok_x = swap(tok, "col")
        tok_y = swap(tok, "depth")
        tok_own = cores(tok)
        w1_cols = cores(w_in)
        w2_rows = cores(w_out)
        grad_own = cores(grad)
        w2_own = part(w2_rows, 2 * c + r, ffn, 0)
        w2_fwd = part(w2_rows, 4 * (1 - c) + 2 * r + d, half, 0)
        w2_a = swap(w2_fwd, "col")
        w2_b = swap(w2_a, "depth")
        grad_x = swap(after(grad, w2_fwd), "col")
        grad_y = swap(after(grad, w2_a), "depth")
        tok_xy = swap(tok_x, "depth")
        grad_xy = swap(grad_x, "depth")

        def w1_part(idx):
            return lax.dynamic_slice(w1_cols, (idx * hid, r * ffn), (hid, ffn))

        pre_own = dot(tok_own, w1_part(c), 1, 0)
        x_near = cores(join_cols(after(tok, pre_own), tok_x, c))
        pre = pre_own + dot(part(x_near, 1 - c, hid, 1), w1_part(1 - c), 1, 0)
        a_near = gelu_tanh(pre).astype(jnp.bfloat16)
        da_own = dot(w2_own, after(grad_own, a_near), 1, 1)
        y_own = dot(after(a_near, da_own), w2_own, 1, 0)
        dw2_near = dot(after(a_near, y_own), grad_own, 0, 0)
        w2_oth = lay_rows((w2_a, after(w2_b, dw2_near)), jnp.stack((d, 1 - d)) * (half // 512), ffn, 512)
        y_oth = dot(a_near, w2_oth, 1, 0)

        def over_cores(v):
            return lax.psum_scatter(v, "row", scatter_dimension=0, tiled=True)

        y_got = swap(over_cores(y_oth), "col")
        y_mine = over_cores(after(y_own, y_oth))
        g_near = cores(join_cols(after(grad, y_oth), grad_x, c))
        d_hidden = da_own.T + dot(part(g_near, 1 - c, hid, 1), w2_oth, 1, 1)
        du_near = jax.vjp(gelu_tanh, pre)[1](d_hidden)[0].astype(jnp.bfloat16)
        dx_oth = dot(du_near, w1_part(1 - c), 1, 1)
        dx_got = swap(over_cores(dx_oth), "col")
        dx_own = dot(after(du_near, dx_oth), w1_part(c), 1, 1)
        dx_mine = over_cores(dx_own)

        x_far = cores(join_cols(after(tok_y, a_near), tok_xy, c))
        w1 = part(w1_cols, r, ffn, 1)
        w2 = join_cols(w2_own, after(w2_oth, y_oth), c)
        pre_far = dot(after(x_far, dx_own), w1, 1, 0)
        a_far = gelu_tanh(pre_far).astype(jnp.bfloat16)
        g_far = cores(join_cols(after(grad_y, a_far), grad_xy, c))

        def dw1_near(idx, dep):
            return dot(part(after(x_near, dep), idx, hid, 1), du_near, 0, 0)

        def dw1_far(idx, dep):
            return dot(part(after(x_far, dep), idx, hid, 1), du_far, 0, 0)

        dw1_send_near = dw1_near(1 - r, a_far)
        du_far = jax.vjp(gelu_tanh, pre_far)[1](dot(after(g_far, dw1_send_near), w2, 1, 1))[0].astype(jnp.bfloat16)
        y = (y_mine + after(y_got, du_far)).astype(jnp.bfloat16)

        quarter, eighth = half // 2, half // 4
        sent, dep = [], y
        for q in range(2):
            at = 2 * d + q
            near = dot(part(after(a_near, dep), at, quarter, 1), part(g_near, 1 - c, hid, 1), 0, 0)
            dep = near + dot(part(a_far, at, quarter, 1), part(g_far, 1 - c, hid, 1), 0, 0)
            sent += [swap(dep[k * eighth:(k + 1) * eighth], "col") for k in range(2)]
        dw2_own = dw2_near + dot(after(a_far, dep), part(g_far, c, hid, 1), 0, 0)
        own_core = swap(dw2_own, "row")
        dw1_send = dw1_send_near + dw1_far(1 - r, dw2_own)
        dw1_got = swap(dw1_send, "row")
        dx = (dx_mine + after(dx_got, dw1_send)).astype(jnp.bfloat16)
        dw1_keep_near = dw1_near(r, dx)
        dw1_keep = dw1_keep_near + dw1_far(r, dw1_keep_near)
        dw1 = join_cols(dw1_keep, dw1_got, r)

        sent2 = [swap(v, "depth") for v in sent]
        oth = sent + sent2
        oth_core = [swap(v, "row") for v in oth]
        inner = jnp.concatenate((4 * d + jnp.arange(4), 4 - 4 * d + jnp.arange(4)))
        dw2 = lay_dw2(dw2_own, own_core, oth, oth_core, c == r, r, inner)
        return y, dx, dw1, dw2

    return jax.shard_map(step_body, mesh=mesh, in_specs=(act_spec, weight_spec, weight_spec, act_spec), out_specs=(act_spec, act_spec, weight_spec, weight_spec), check_vma=False)
```

```python
import jax
import jax.numpy as jnp
from jax import lax
from jax.experimental import pallas as pl
from jax.experimental.pallas import tpu as pltpu
from jax.sharding import PartitionSpec as P


SWAP = [(0, 1), (1, 0)]


def gelu_tanh(pre_act):
    return jax.nn.gelu(pre_act, approximate=True)


def dot(lhs, rhs, lc, rc):
    return lax.dot_general(lhs, rhs, (((lc,), (rc,)), ((), ())), preferred_element_type=jnp.float32)


def part(arr, idx, size, axis):
    return lax.dynamic_slice_in_dim(arr, idx * size, size, axis)


def after(val, *deps):
    return lax.optimization_barrier((val,) + deps)[0]


def lay(pieces, out_rows, out_cols, step, first=None, blocks=None, onto=None):
    cols, dtype = out_cols, pieces[0][0].dtype
    width = next(iter({p[4][1] for p in pieces}))
    per_col = out_rows // step
    sizes = [p[2] // step for p in pieces]
    n = len(pieces)
    table = [p[1] for p in pieces] + [p[3] // step for p in pieces] + [p[4][0] for p in pieces]
    runs = 0
    if onto is not None:
        table += list(first)
        runs = blocks
        total = len(first) * blocks
    else:
        total = per_col * (cols // width)
    table = jnp.stack([jnp.asarray(v, jnp.int32) for v in table])

    def where_to(at, tab):
        if onto is None:
            return at
        pos = tab[3 * n] + at
        for k in range(1, len(first)):
            pos = jnp.where(at >= k * runs, tab[3 * n + k] + at - k * runs, pos)
        return pos

    def body(tab, *refs):
        out_ref = refs[-1]
        pos = where_to(pl.program_id(0), tab)
        for k, size in enumerate(sizes):
            @pl.when((tab[k] >= 0) & (pos >= tab[k]) & (pos < tab[k] + size))
            def _(k=k):
                out_ref[...] = refs[k][...]

    def in_map(k, size):
        def index(at, tab):
            here = jnp.where(tab[k] < 0, 0, jnp.clip(where_to(at, tab) - tab[k], 0, size - 1))
            return (tab[n + k] + here, tab[2 * n + k])

        return index

    def out_map(at, tab):
        pos = where_to(at, tab)
        return (lax.rem(pos, per_col), lax.div(pos, per_col))

    in_specs = [pl.BlockSpec((step, width), in_map(k, size)) for k, size in enumerate(sizes)]
    operands = [p[0] for p in pieces]
    aliases = {}
    if onto is not None:
        in_specs.append(pl.BlockSpec(memory_space=pl.ANY))
        operands.append(onto)
        aliases = {n + 1: 0}
    return pl.pallas_call(
        body,
        out_shape=jax.ShapeDtypeStruct((out_rows, out_cols), dtype),
        grid_spec=pltpu.PrefetchScalarGridSpec(
            num_scalar_prefetch=1,
            grid=(total,),
            in_specs=in_specs,
            out_specs=pl.BlockSpec((step, width), out_map),
        ),
        input_output_aliases=aliases,
        cost_estimate=pl.CostEstimate(flops=total * step * width * 400, bytes_accessed=2 * total * step * width * dtype.itemsize, transcendentals=0),
    )(table, *operands)


def whole(arr, place):
    return (arr, place, arr.shape[0], 0, (0, arr.shape[1]))


def join_cols(mine, other, idx, step):
    per = mine.shape[0] // step
    return lay([whole(mine, idx * per), whole(other, (1 - idx) * per)], mine.shape[0], 2 * mine.shape[1], step)


def solution(mesh):
    act_spec = P(("depth", "row"), "col")
    weight_spec = P("row", "col")

    def step_body(tok, w_in, w_out, grad):
        d, c, r = lax.axis_index("depth"), lax.axis_index("col"), lax.axis_index("row")
        hid = tok.shape[1]
        ffn = w_in.shape[1] // 2
        half, quarter, eighth = ffn // 2, ffn // 4, ffn // 8
        stay = c == r

        def swap(v, axis):
            return lax.ppermute(v, axis, SWAP)

        def cores(v):
            return lax.all_gather(v, "row", axis=0, tiled=True)

        def over_cores(v):
            return lax.psum_scatter(v, "row", scatter_dimension=0, tiled=True)

        tok_x = swap(tok, "col")
        tok_y = swap(tok, "depth")
        tok_own = cores(tok)
        grad_own = cores(grad)

        w2_cut = part(w_out, 1 - r, ffn, 0)
        w1_cut = part(w_in, 1 - r, ffn, 1)
        w2_core = swap(w2_cut, "row")
        w1_core = swap(w1_cut, "row")
        step = 512
        w2_fwd = lay([(w_out, jnp.where(stay, -1, 0), half, r * ffn + d * half, (0, hid)), (w2_core, jnp.where(stay, 0, -1), half, d * half, (0, hid))], half, hid, step)
        per1 = hid // 256
        w1 = lay([(w_in, r * per1, hid, 0, (r, ffn)), whole(w1_core, (1 - r) * per1)], 2 * hid, ffn, 256)
        w2_a = swap(w2_fwd, "col")
        grad_x = swap(after(grad, w2_fwd), "col")
        tok_xy = swap(tok_x, "depth")
        w2_b = swap(w2_a, "depth")
        grad_y = swap(after(grad, w2_a), "depth")
        grad_xy = swap(grad_x, "depth")

        def with_slope(pre):
            hidden, back = jax.vjp(gelu_tanh, pre)
            return hidden.astype(jnp.bfloat16), back(jnp.ones_like(pre))[0]

        pre_own = dot(tok_own, part(w1, c, hid, 0), 1, 0)
        tok_oth = cores(after(tok_x, pre_own))
        w2_own = lay([(w_out, jnp.where(stay, 0, -1), ffn, r * ffn, (0, hid)), (after(w2_core, pre_own), jnp.where(stay, -1, 0), ffn, 0, (0, hid))], ffn, hid, step)
        pre = pre_own + dot(after(tok_oth, w2_own), part(w1, 1 - c, hid, 0), 1, 0)
        a_near, slope_near = lax.optimization_barrier(with_slope(pre))
        x_far = cores(join_cols(after(tok_y, a_near), tok_xy, c, step))
        da_own = dot(w2_own, after(grad_own, a_near), 1, 1)
        x_near = cores(join_cols(after(tok, da_own), tok_x, c, step))
        a_far, slope_far = lax.optimization_barrier(with_slope(dot(after(x_far, da_own), w1, 1, 0)))
        per2 = ffn // step
        w2 = lay([whole(w2_own, c * per2), whole(w2_a, (1 - c) * per2 + d * (per2 // 2)), whole(after(w2_b, a_far), (1 - c) * per2 + (1 - d) * (per2 // 2))], ffn, 2 * hid, step)
        y_oth = dot(a_near, part(w2, 1 - c, hid, 1), 1, 0)
        y_got = swap(over_cores(y_oth), "col")
        grad_oth = cores(after(grad_x, y_oth))
        d_hidden = da_own.T + dot(grad_oth, part(w2, 1 - c, hid, 1), 1, 1)
        du_near = (slope_near * d_hidden).astype(jnp.bfloat16)
        dx_oth = dot(du_near, part(w1, 1 - c, hid, 0), 1, 1)
        dx_got = swap(over_cores(dx_oth), "col")
        g_far = cores(join_cols(after(grad_y, dx_oth), grad_xy, c, step))
        y_own = dot(after(a_near, dx_oth), part(w2, c, hid, 1), 1, 0)
        y_mine = over_cores(y_own)
        du_far = (slope_far * dot(after(g_far, y_own), w2, 1, 1)).astype(jnp.bfloat16)

        sent, dep = [], du_far
        for q in range(2):
            near = dot(part(after(a_near, dep), 2 * d + q, quarter, 1), grad_oth, 0, 0)
            dep = near + dot(part(a_far, 2 * d + q, quarter, 1), part(g_far, 1 - c, hid, 1), 0, 0)
            sent += [swap(dep[k * eighth:(k + 1) * eighth], "col") for k in range(2)]
        dx_own = dot(after(du_near, dep), part(w1, c, hid, 0), 1, 1)
        dx_mine = over_cores(dx_own)
        dw2_near = dot(after(a_near, dx_own), grad_own, 0, 0)
        dw2_own = dw2_near + dot(after(a_far, dw2_near), part(g_far, c, hid, 1), 0, 0)
        own_core = swap(dw2_own, "row")
        y = (y_mine + after(y_got, dw2_own)).astype(jnp.bfloat16)

        def dw1_near(idx, dep):
            return dot(part(after(x_near, dep), idx, hid, 1), du_near, 0, 0)

        def dw1_far(idx, dep):
            return dot(part(after(x_far, dep), idx, hid, 1), du_far, 0, 0)

        dw1_send_near = dw1_near(1 - r, y)
        dw1_send = dw1_send_near + dw1_far(1 - r, dw1_send_near)
        dw1_got = swap(dw1_send, "row")
        dx = (dx_mine + after(dx_got, dw1_send)).astype(jnp.bfloat16)
        dw1_keep_near = dw1_near(r, dx)
        dw1_keep = dw1_keep_near + dw1_far(r, dw1_keep_near)
        dw1 = join_cols(dw1_keep, dw1_got, r, 256)

        sent2 = [swap(v, "depth") for v in sent]
        sent_core = [swap(v, "row") for v in sent]
        sent2_core = [swap(v, "row") for v in sent2]
        dstep = 256
        slot, run, size = ffn // dstep, half // dstep, eighth // dstep

        def pieces(mine, core, at):
            own = [whole(dw2_own, jnp.where(stay, slot * r, -1)), whole(own_core, jnp.where(stay, slot * (1 - r), -1))]
            mine = [whole(v, jnp.where(stay, -1, slot * r + run * at + size * k)) for k, v in enumerate(mine)]
            return own + mine + [whole(v, jnp.where(stay, -1, slot * (1 - r) + run * at + size * k)) for k, v in enumerate(core)]

        dw2 = lay(pieces([after(v, dw1) for v in sent], sent_core, d), 2 * ffn, hid, dstep)
        dw2 = lay(pieces(sent2, sent2_core, 1 - d), 2 * ffn, hid, dstep, first=(slot * r + run * (1 - d), slot * (1 - r) + run * (1 - d)), blocks=run, onto=dw2)
        return y, dx, dw1, dw2

    return jax.shard_map(step_body, mesh=mesh, in_specs=(act_spec, weight_spec, weight_spec, act_spec), out_specs=(act_spec, act_spec, weight_spec, weight_spec), check_vma=False)
```

```python
import math

import jax
import jax.numpy as jnp
from jax import lax
from jax.experimental import pallas as pl
from jax.experimental.pallas import tpu as pltpu
from jax.sharding import PartitionSpec as P


SWAP = [(0, 1), (1, 0)]


def gelu_tanh(pre_act):
    return jax.nn.gelu(pre_act, approximate=True)


def dot(lhs, rhs, lc, rc):
    return lax.dot_general(lhs, rhs, (((lc,), (rc,)), ((), ())), preferred_element_type=jnp.float32)


def part(arr, idx, size, axis):
    return lax.dynamic_slice_in_dim(arr, idx * size, size, axis)


def after(val, *deps):
    return lax.optimization_barrier((val,) + deps)[0]


def lay(pieces, out_rows, out_cols, step, first=None, blocks=None, onto=None):
    cols, dtype = out_cols, pieces[0][0].dtype
    width = next(iter({p[4][1] for p in pieces}))
    per_col = out_rows // step
    sizes = [p[2] // step for p in pieces]
    n = len(pieces)
    table = [p[1] for p in pieces] + [p[3] // step for p in pieces] + [p[4][0] for p in pieces]
    runs = 0
    if onto is not None:
        table += list(first)
        runs = blocks
        total = len(first) * blocks
    else:
        total = per_col * (cols // width)
    table = jnp.stack([jnp.asarray(v, jnp.int32) for v in table])

    def where_to(at, tab):
        if onto is None:
            return at
        pos = tab[3 * n] + at
        for k in range(1, len(first)):
            pos = jnp.where(at >= k * runs, tab[3 * n + k] + at - k * runs, pos)
        return pos

    def body(tab, *refs):
        out_ref = refs[-1]
        pos = where_to(pl.program_id(0), tab)
        for k, size in enumerate(sizes):
            @pl.when((tab[k] >= 0) & (pos >= tab[k]) & (pos < tab[k] + size))
            def _(k=k):
                out_ref[...] = refs[k][...]

    def in_map(k, size):
        def index(at, tab):
            here = jnp.where(tab[k] < 0, 0, jnp.clip(where_to(at, tab) - tab[k], 0, size - 1))
            return (tab[n + k] + here, tab[2 * n + k])

        return index

    def out_map(at, tab):
        pos = where_to(at, tab)
        return (lax.rem(pos, per_col), lax.div(pos, per_col))

    in_specs = [pl.BlockSpec((step, width), in_map(k, size)) for k, size in enumerate(sizes)]
    operands = [p[0] for p in pieces]
    aliases = {}
    if onto is not None:
        in_specs.append(pl.BlockSpec(memory_space=pl.ANY))
        operands.append(onto)
        aliases = {n + 1: 0}
    return pl.pallas_call(
        body,
        out_shape=jax.ShapeDtypeStruct((out_rows, out_cols), dtype),
        grid_spec=pltpu.PrefetchScalarGridSpec(
            num_scalar_prefetch=1,
            grid=(total,),
            in_specs=in_specs,
            out_specs=pl.BlockSpec((step, width), out_map),
        ),
        input_output_aliases=aliases,
        cost_estimate=pl.CostEstimate(flops=total * step * width * 400, bytes_accessed=2 * total * step * width * dtype.itemsize, transcendentals=0),
    )(table, *operands)


def whole(arr, place):
    return (arr, place, arr.shape[0], 0, (0, arr.shape[1]))


def join_cols(mine, other, idx, step):
    per = mine.shape[0] // step
    return lay([whole(mine, idx * per), whole(other, (1 - idx) * per)], mine.shape[0], 2 * mine.shape[1], step)


def gelu_and_slope(pre):
    scale, cubic = (2.0 / math.pi) ** 0.5, 0.044715
    square = pre * pre
    tanh = jnp.tanh(pre * (scale + (scale * cubic) * square))
    cdf = 0.5 + 0.5 * tanh
    return pre * cdf, cdf + (0.5 * pre) * (1.0 - tanh * tanh) * (scale + (3.0 * scale * cubic) * square)


def ffn_kernel(grad, w2, pre=None, x=None, w1=None):
    rows, ffn, depth = grad.shape[0], w2.shape[0], grad.shape[1]
    tm, tn, sub = 512, 1024, 256
    fused = pre is None

    def body(*refs):
        grad_ref, w2_ref = refs[0], refs[1]
        du_ref = refs[-1]
        for at in range(0, tn, sub):
            cols = slice(at, at + sub)
            if fused:
                u = jnp.dot(refs[2][...], refs[3][:, cols], preferred_element_type=jnp.float32)
            else:
                u = refs[2][:, cols]
            d_hidden = dot(grad_ref[...], w2_ref[cols, :], 1, 1)
            hidden, slope = gelu_and_slope(u)
            if fused:
                refs[4][:, cols] = hidden.astype(jnp.bfloat16)
            du_ref[:, cols] = (slope * d_hidden).astype(jnp.bfloat16)

    out = jax.ShapeDtypeStruct((rows, ffn), jnp.bfloat16)
    tile = pl.BlockSpec((tm, tn), lambda j, i: (i, j))
    tall = pl.BlockSpec((tm, depth), lambda j, i: (i, 0))
    in_specs = [tall, pl.BlockSpec((tn, depth), lambda j, i: (j, 0))]
    in_specs += [tall, pl.BlockSpec((depth, tn), lambda j, i: (0, j))] if fused else [tile]
    flops = 2 * rows * ffn * depth * (2 if fused else 1)
    return pl.pallas_call(
        body,
        grid=(ffn // tn, rows // tm),
        in_specs=in_specs,
        out_specs=[tile] * (2 if fused else 1),
        out_shape=[out] * (2 if fused else 1),
        compiler_params=pltpu.CompilerParams(vmem_limit_bytes=56 * 1024 * 1024),
        cost_estimate=pl.CostEstimate(flops=flops, bytes_accessed=6 * rows * ffn, transcendentals=rows * ffn),
    )(*((grad, w2, x, w1) if fused else (grad, w2, pre)))


def solution(mesh):
    act_spec = P(("depth", "row"), "col")
    weight_spec = P("row", "col")

    def step_body(tok, w_in, w_out, grad):
        d, c, r = lax.axis_index("depth"), lax.axis_index("col"), lax.axis_index("row")
        hid = tok.shape[1]
        ffn = w_in.shape[1] // 2
        half, quarter, eighth = ffn // 2, ffn // 4, ffn // 8
        stay = c == r

        def swap(v, axis):
            return lax.ppermute(v, axis, SWAP)

        def cores(v):
            return lax.all_gather(v, "row", axis=0, tiled=True)

        def over_cores(v):
            return lax.psum_scatter(v, "row", scatter_dimension=0, tiled=True)

        tok_x = swap(tok, "col")
        tok_y = swap(tok, "depth")
        tok_own = cores(tok)
        grad_own = cores(grad)

        w2_cut = part(w_out, 1 - r, ffn, 0)
        w1_cut = part(w_in, 1 - r, ffn, 1)
        w2_core = swap(w2_cut, "row")
        w1_core = swap(w1_cut, "row")
        step = 1024
        w2_fwd = lay([(w_out, jnp.where(stay, -1, 0), half, r * ffn + d * half, (0, hid)), (w2_core, jnp.where(stay, 0, -1), half, d * half, (0, hid))], half, hid, step)
        per1 = hid // 256
        w1 = lay([(w_in, r * per1, hid, 0, (r, ffn)), whole(w1_core, (1 - r) * per1)], 2 * hid, ffn, 256)
        w2_a = swap(w2_fwd, "col")
        grad_x = swap(after(grad, w2_fwd), "col")
        tok_xy = swap(tok_x, "depth")
        w2_b = swap(w2_a, "depth")
        grad_y = swap(after(grad, w2_a), "depth")
        grad_xy = swap(grad_x, "depth")

        pre_own = dot(tok_own, part(w1, c, hid, 0), 1, 0)
        tok_oth = cores(after(tok_x, pre_own))
        w2_own = lay([(w_out, jnp.where(stay, 0, -1), ffn, r * ffn, (0, hid)), (after(w2_core, pre_own), jnp.where(stay, -1, 0), ffn, 0, (0, hid))], ffn, hid, step)
        pre = pre_own + dot(after(tok_oth, w2_own), part(w1, 1 - c, hid, 0), 1, 0)
        a_near, pre = lax.optimization_barrier((gelu_tanh(pre).astype(jnp.bfloat16), pre))
        y_own = dot(a_near, w2_own, 1, 0)
        dw2_near = dot(after(a_near, y_own), grad_own, 0, 0)
        g_near = cores(join_cols(after(grad, dw2_near), grad_x, c, step))
        per2 = ffn // step
        w2 = lay([whole(w2_own, c * per2), whole(w2_a, (1 - c) * per2 + d * (per2 // 2)), whole(after(w2_b, dw2_near), (1 - c) * per2 + (1 - d) * (per2 // 2))], ffn, 2 * hid, step)
        y_oth = dot(a_near, part(w2, 1 - c, hid, 1), 1, 0)
        y_got = swap(over_cores(y_oth), "col")
        x_far = cores(join_cols(after(tok_y, y_oth), tok_xy, c, step))
        (du_near,) = ffn_kernel(after(g_near, y_oth), w2, pre=pre)
        y_mine = over_cores(after(y_own, du_near))
        dx_oth = dot(du_near, part(w1, 1 - c, hid, 0), 1, 1)
        dx_got = swap(over_cores(dx_oth), "col")
        g_far = cores(join_cols(after(grad_y, dx_oth), grad_xy, c, step))
        dx_own = dot(after(du_near, dx_oth), part(w1, c, hid, 0), 1, 1)
        x_near = cores(join_cols(after(tok, dx_own), tok_x, c, step))
        dx_mine = over_cores(dx_own)
        a_far, du_far = ffn_kernel(after(g_far, dx_own), w2, x=x_far, w1=w1)

        sent, dep = [], du_far
        for q in range(2):
            near = dot(part(after(a_near, dep), 2 * d + q, quarter, 1), part(g_near, 1 - c, hid, 1), 0, 0)
            dep = near + dot(part(a_far, 2 * d + q, quarter, 1), part(g_far, 1 - c, hid, 1), 0, 0)
            sent += [swap(dep[k * eighth:(k + 1) * eighth], "col") for k in range(2)]
        dw2_own = dw2_near + dot(after(a_far, dep), part(g_far, c, hid, 1), 0, 0)
        own_core = swap(dw2_own, "row")
        y = (y_mine + after(y_got, dw2_own)).astype(jnp.bfloat16)

        def dw1_near(idx, dep):
            return dot(part(after(x_near, dep), idx, hid, 1), du_near, 0, 0)

        def dw1_far(idx, dep):
            return dot(part(after(x_far, dep), idx, hid, 1), du_far, 0, 0)

        dw1_send_near = dw1_near(1 - r, y)
        dw1_send = dw1_send_near + dw1_far(1 - r, dw1_send_near)
        dw1_got = swap(dw1_send, "row")
        dx = (dx_mine + after(dx_got, dw1_send)).astype(jnp.bfloat16)
        dw1_keep_near = dw1_near(r, dx)
        dw1_keep = dw1_keep_near + dw1_far(r, dw1_keep_near)
        dw1 = join_cols(dw1_keep, dw1_got, r, 256)

        sent2 = [swap(v, "depth") for v in sent]
        sent_core = [swap(v, "row") for v in sent]
        sent2_core = [swap(v, "row") for v in sent2]
        dstep = 512
        slot, run, size = ffn // dstep, half // dstep, eighth // dstep

        def pieces(mine, core, at):
            own = [whole(dw2_own, jnp.where(stay, slot * r, -1)), whole(own_core, jnp.where(stay, slot * (1 - r), -1))]
            mine = [whole(v, jnp.where(stay, -1, slot * r + run * at + size * k)) for k, v in enumerate(mine)]
            return own + mine + [whole(v, jnp.where(stay, -1, slot * (1 - r) + run * at + size * k)) for k, v in enumerate(core)]

        dw2 = lay(pieces([after(v, dw1) for v in sent], sent_core, d), 2 * ffn, hid, dstep)
        dw2 = lay(pieces(sent2, sent2_core, 1 - d), 2 * ffn, hid, dstep, first=(slot * r + run * (1 - d), slot * (1 - r) + run * (1 - d)), blocks=run, onto=dw2)
        return y, dx, dw1, dw2

    return jax.shard_map(step_body, mesh=mesh, in_specs=(act_spec, weight_spec, weight_spec, act_spec), out_specs=(act_spec, act_spec, weight_spec, weight_spec), check_vma=False)
```

```python
import math

import jax
import jax.numpy as jnp
from jax import lax
from jax.experimental import pallas as pl
from jax.experimental.pallas import tpu as pltpu
from jax.sharding import PartitionSpec as P


SWAP = [(0, 1), (1, 0)]


def gelu_tanh(pre_act):
    return jax.nn.gelu(pre_act, approximate=True)


def dot(lhs, rhs, lc, rc):
    return lax.dot_general(lhs, rhs, (((lc,), (rc,)), ((), ())), preferred_element_type=jnp.float32)


def part(arr, idx, size, axis):
    return lax.dynamic_slice_in_dim(arr, idx * size, size, axis)


def after(val, *deps):
    return lax.optimization_barrier((val,) + deps)[0]


def lay(pieces, out_rows, out_cols, step, first=None, blocks=None, onto=None):
    cols, dtype = out_cols, pieces[0][0].dtype
    width = next(iter({p[4][1] for p in pieces}))
    per_col = out_rows // step
    sizes = [p[2] // step for p in pieces]
    n = len(pieces)
    table = [p[1] for p in pieces] + [p[3] // step for p in pieces] + [p[4][0] for p in pieces]
    runs = 0
    if onto is not None:
        table += list(first)
        runs = blocks
        total = len(first) * blocks
    else:
        total = per_col * (cols // width)
    table = jnp.stack([jnp.asarray(v, jnp.int32) for v in table])

    def where_to(at, tab):
        if onto is None:
            return at
        pos = tab[3 * n] + at
        for k in range(1, len(first)):
            pos = jnp.where(at >= k * runs, tab[3 * n + k] + at - k * runs, pos)
        return pos

    def body(tab, *refs):
        out_ref = refs[-1]
        pos = where_to(pl.program_id(0), tab)
        for k, size in enumerate(sizes):
            @pl.when((tab[k] >= 0) & (pos >= tab[k]) & (pos < tab[k] + size))
            def _(k=k):
                out_ref[...] = refs[k][...]

    def in_map(k, size):
        def index(at, tab):
            here = jnp.where(tab[k] < 0, 0, jnp.clip(where_to(at, tab) - tab[k], 0, size - 1))
            return (tab[n + k] + here, tab[2 * n + k])

        return index

    def out_map(at, tab):
        pos = where_to(at, tab)
        return (lax.rem(pos, per_col), lax.div(pos, per_col))

    in_specs = [pl.BlockSpec((step, width), in_map(k, size)) for k, size in enumerate(sizes)]
    operands = [p[0] for p in pieces]
    aliases = {}
    if onto is not None:
        in_specs.append(pl.BlockSpec(memory_space=pl.ANY))
        operands.append(onto)
        aliases = {n + 1: 0}
    return pl.pallas_call(
        body,
        out_shape=jax.ShapeDtypeStruct((out_rows, out_cols), dtype),
        grid_spec=pltpu.PrefetchScalarGridSpec(
            num_scalar_prefetch=1,
            grid=(total,),
            in_specs=in_specs,
            out_specs=pl.BlockSpec((step, width), out_map),
        ),
        input_output_aliases=aliases,
        cost_estimate=pl.CostEstimate(flops=total * step * width * 400, bytes_accessed=2 * total * step * width * dtype.itemsize, transcendentals=0),
    )(table, *operands)


def whole(arr, place):
    return (arr, place, arr.shape[0], 0, (0, arr.shape[1]))


def join_cols(mine, other, idx, step):
    per = mine.shape[0] // step
    return lay([whole(mine, idx * per), whole(other, (1 - idx) * per)], mine.shape[0], 2 * mine.shape[1], step)


def gelu_and_slope(pre):
    scale, cubic = (2.0 / math.pi) ** 0.5, 0.044715
    square = pre * pre
    tanh = jnp.tanh(pre * (scale + (scale * cubic) * square))
    cdf = 0.5 + 0.5 * tanh
    return pre * cdf, cdf + (0.5 * pre) * (1.0 - tanh * tanh) * (scale + (3.0 * scale * cubic) * square)


def ffn_kernel(grad, w2, pre=None, x=None, w1=None):
    rows, ffn, depth = grad.shape[0], w2.shape[0], grad.shape[1]
    tm, tn, sub = 512, 1024, 256
    fused = pre is None

    def body(*refs):
        grad_ref, w2_ref = refs[0], refs[1]
        du_ref = refs[-1]
        for at in range(0, tn, sub):
            cols = slice(at, at + sub)
            if fused:
                u = jnp.dot(refs[2][...], refs[3][:, cols], preferred_element_type=jnp.float32)
            else:
                u = refs[2][:, cols]
            d_hidden = dot(grad_ref[...], w2_ref[cols, :], 1, 1)
            hidden, slope = gelu_and_slope(u)
            if fused:
                refs[4][:, cols] = hidden.astype(jnp.bfloat16)
            du_ref[:, cols] = (slope * d_hidden).astype(jnp.bfloat16)

    out = jax.ShapeDtypeStruct((rows, ffn), jnp.bfloat16)
    tile = pl.BlockSpec((tm, tn), lambda j, i: (i, j))
    tall = pl.BlockSpec((tm, depth), lambda j, i: (i, 0))
    in_specs = [tall, pl.BlockSpec((tn, depth), lambda j, i: (j, 0))]
    in_specs += [tall, pl.BlockSpec((depth, tn), lambda j, i: (0, j))] if fused else [tile]
    flops = 2 * rows * ffn * depth * (2 if fused else 1)
    return pl.pallas_call(
        body,
        grid=(ffn // tn, rows // tm),
        in_specs=in_specs,
        out_specs=[tile] * (2 if fused else 1),
        out_shape=[out] * (2 if fused else 1),
        compiler_params=pltpu.CompilerParams(vmem_limit_bytes=56 * 1024 * 1024),
        cost_estimate=pl.CostEstimate(flops=flops, bytes_accessed=6 * rows * ffn, transcendentals=rows * ffn),
    )(*((grad, w2, x, w1) if fused else (grad, w2, pre)))


def solution(mesh):
    act_spec = P(("depth", "row"), "col")
    weight_spec = P("row", "col")

    def step_body(tok, w_in, w_out, grad):
        d, c, r = lax.axis_index("depth"), lax.axis_index("col"), lax.axis_index("row")
        hid = tok.shape[1]
        ffn = w_in.shape[1] // 2
        half, quarter, eighth = ffn // 2, ffn // 4, ffn // 8
        stay = c == r

        def swap(v, axis):
            return lax.ppermute(v, axis, SWAP)

        def cores(v):
            return lax.all_gather(v, "row", axis=0, tiled=True)

        def over_cores(v):
            return lax.psum_scatter(v, "row", scatter_dimension=0, tiled=True)

        tok_x = swap(tok, "col")
        tok_y = swap(tok, "depth")
        tok_own = cores(tok)
        grad_own = cores(grad)

        w2_cut = part(w_out, 1 - r, ffn, 0)
        w1_cut = part(w_in, 1 - r, ffn, 1)
        w2_core = swap(w2_cut, "row")
        w1_core = swap(w1_cut, "row")
        step = 1024
        per1 = hid // 256
        w1 = lay([(w_in, r * per1, hid, 0, (r, ffn)), whole(w1_core, (1 - r) * per1)], 2 * hid, ffn, 256)
        w2_core = after(w2_core, w1)
        w2_fwd = lay([(w_out, jnp.where(stay, -1, 0), half, r * ffn + d * half, (0, hid)), (w2_core, jnp.where(stay, 0, -1), half, d * half, (0, hid))], half, hid, step)
        w2_a = swap(w2_fwd, "col")
        grad_x = swap(after(grad, w2_fwd), "col")
        tok_xy = swap(tok_x, "depth")
        w2_b = swap(w2_a, "depth")
        grad_y = swap(after(grad, w2_a), "depth")
        grad_xy = swap(grad_x, "depth")

        pre_own = dot(tok_own, part(w1, c, hid, 0), 1, 0)
        tok_oth = cores(after(tok_x, pre_own))
        w2_own = lay([(w_out, jnp.where(stay, 0, -1), ffn, r * ffn, (0, hid)), (after(w2_core, pre_own), jnp.where(stay, -1, 0), ffn, 0, (0, hid))], ffn, hid, step)
        pre = pre_own + dot(after(tok_oth, w2_own), part(w1, 1 - c, hid, 0), 1, 0)
        a_near, pre = lax.optimization_barrier((gelu_tanh(pre).astype(jnp.bfloat16), pre))
        y_own = dot(a_near, w2_own, 1, 0)
        dw2_near = dot(after(a_near, y_own), grad_own, 0, 0)
        g_near = cores(join_cols(after(grad, dw2_near), grad_x, c, step))
        per2 = ffn // step
        w2 = lay([whole(w2_own, c * per2), whole(w2_a, (1 - c) * per2 + d * (per2 // 2)), whole(after(w2_b, dw2_near), (1 - c) * per2 + (1 - d) * (per2 // 2))], ffn, 2 * hid, step)
        y_oth = dot(a_near, part(w2, 1 - c, hid, 1), 1, 0)
        y_got = swap(over_cores(y_oth), "col")
        tok_far = join_cols(after(tok_y, y_oth), tok_xy, c, step)
        x_far = cores(tok_far)
        (du_near,) = ffn_kernel(after(g_near, y_oth, tok_far), w2, pre=pre)
        y_mine = over_cores(after(y_own, du_near))
        dx_oth = dot(du_near, part(w1, 1 - c, hid, 0), 1, 1)
        dx_got = swap(over_cores(dx_oth), "col")
        g_far = cores(join_cols(after(grad_y, dx_oth), grad_xy, c, step))
        dx_own = dot(after(du_near, dx_oth), part(w1, c, hid, 0), 1, 1)
        x_near = cores(join_cols(after(tok, dx_own), tok_x, c, step))
        dx_mine = over_cores(dx_own)
        a_far, du_far = ffn_kernel(after(g_far, dx_own), w2, x=x_far, w1=w1)

        sent, dep = [], du_far
        for q in range(2):
            near = dot(part(after(a_near, dep), 2 * d + q, quarter, 1), part(g_near, 1 - c, hid, 1), 0, 0)
            dep = near + dot(part(a_far, 2 * d + q, quarter, 1), part(g_far, 1 - c, hid, 1), 0, 0)
            sent += [swap(dep[k * eighth:(k + 1) * eighth], "col") for k in range(2)]
        dw2_own = dw2_near + dot(after(a_far, dep), part(g_far, c, hid, 1), 0, 0)
        own_core = swap(dw2_own, "row")
        y = (y_mine + after(y_got, dw2_own)).astype(jnp.bfloat16)

        def dw1_near(idx, dep):
            return dot(part(after(x_near, dep), idx, hid, 1), du_near, 0, 0)

        def dw1_far(idx, dep):
            return dot(part(after(x_far, dep), idx, hid, 1), du_far, 0, 0)

        dw1_send_near = dw1_near(1 - r, y)
        dw1_send = dw1_send_near + dw1_far(1 - r, dw1_send_near)
        dw1_got = swap(dw1_send, "row")
        dx = (dx_mine + after(dx_got, dw1_send)).astype(jnp.bfloat16)
        dw1_keep_near = dw1_near(r, dx)
        dw1_keep = dw1_keep_near + dw1_far(r, dw1_keep_near)
        dw1 = join_cols(dw1_keep, dw1_got, r, 256)

        sent2 = [swap(v, "depth") for v in sent]
        sent_core = [swap(v, "row") for v in sent]
        sent2_core = [swap(v, "row") for v in sent2]
        dstep = 512
        slot, run, size = ffn // dstep, half // dstep, eighth // dstep

        def pieces(mine, core, at):
            own = [whole(dw2_own, jnp.where(stay, slot * r, -1)), whole(own_core, jnp.where(stay, slot * (1 - r), -1))]
            mine = [whole(v, jnp.where(stay, -1, slot * r + run * at + size * k)) for k, v in enumerate(mine)]
            return own + mine + [whole(v, jnp.where(stay, -1, slot * (1 - r) + run * at + size * k)) for k, v in enumerate(core)]

        dw2 = lay(pieces([after(v, dw1) for v in sent], sent_core, d), 2 * ffn, hid, dstep)
        dw2 = lay(pieces(sent2, sent2_core, 1 - d), 2 * ffn, hid, dstep, first=(slot * r + run * (1 - d), slot * (1 - r) + run * (1 - d)), blocks=run, onto=dw2)
        return y, dx, dw1, dw2

    return jax.shard_map(step_body, mesh=mesh, in_specs=(act_spec, weight_spec, weight_spec, act_spec), out_specs=(act_spec, act_spec, weight_spec, weight_spec), check_vma=False)
```
